32 devices in a mesh: grp: 4 (over x, core), dev: 8 (over z, y).
Axes of the slice: x: 2, y: 2, z: 4, core: 2. Of those that a mesh axis runs over, the one named last changes fastest.
Arguments:
- fields: float32 [24, 64, 128, 128], P(None, ('grp', 'dev')), may hold values from -6 to 6
- mix_matrix: float32 [24, 24], replicated, may hold values from -1.25 to 1.25
- laplace_matrix: float32 [24, 24], replicated, may hold values from -0.21875 to 0.21875
Outputs:
- rhs: float32 [24, 64, 128, 128], P(None, ('grp', 'dev'))
- weyl: float32 [2, 64, 128, 128], P(None, 'grp', 'dev')
The draws below stay inside these ranges and needn't reach their ends.
All inputs are finite; a program needn't handle non-finite values.
Results may differ from the reference program's by a relative error of at most 0.0003.
Values sent between devices are 32-bit elements; how exact they have to be, the bound alone decides.
No kernel may reach another device: no remote copies, remote signals or barrier semaphores. Data moves between devices by JAX's collectives and lax.ppermute only.
A program may use at most 192 MiB of HBM per device.

```python
import jax
import jax.numpy as jnp
from jax import lax

FIELDS = 24
CZ = 2
NY = 128
NX = 128
NZ = 64


def block_scale(key, dims, split, smallest, top_value):
    level = 1.0
    for position, blocks in split:
        draws = jax.random.uniform(jax.random.fold_in(jax.random.fold_in(key, 6), position), (blocks,), jnp.float32, smallest / len(split), top_value / len(split))
        level = level * jnp.repeat(jnp.exp(draws), dims[position] // blocks).reshape((-1,) + (1,) * (len(dims) - 1 - position))
    return level


def normal_values(stream_key, shape, scale, reach, split=(), kind=jnp.bfloat16):
    values = scale * jax.random.normal(stream_key, shape, jnp.float32)
    if split:
        values = values * block_scale(stream_key, shape, split, -0.22, 0.18)
    return jnp.clip(values, -reach, reach).astype(kind)


def setup_inputs(seed: int = 0) -> dict:
    keys = jax.random.split(jax.random.key(seed), 4)
    fields = normal_values(keys[0], (FIELDS, NZ, NY, NX), 1.0, 6.0, ((1, 32),), jnp.float32)
    mix_matrix = normal_values(keys[1], (FIELDS, FIELDS), FIELDS ** -0.5, 1.25, (), jnp.float32)
    laplace_matrix = normal_values(keys[2], (FIELDS, FIELDS), (FIELDS * 30) ** -0.5, 0.21875, (), jnp.float32)
    return {"fields": fields, "mix_matrix": mix_matrix, "laplace_matrix": laplace_matrix}


def pad_periodic(field, dimension):
    length = field.shape[dimension]
    before = lax.slice_in_dim(field, length - 2, length, axis=dimension)
    after = lax.slice_in_dim(field, 0, 2, axis=dimension)
    return jnp.concatenate([before, field, after], axis=dimension)

def interior(padded, keep):
    result = padded
    for dimension in (1, 2, 3):
        if dimension != keep:
            result = lax.slice_in_dim(result, 2, result.shape[dimension] - 2, axis=dimension)
    return result

def stencil_values(padded, dimension):
    centre = interior(padded, dimension)
    length = centre.shape[dimension] - 4
    return [lax.slice_in_dim(centre, offset, offset + length, axis=dimension) for offset in range(5)]

def first_diff(padded, dimension):
    values = stencil_values(padded, dimension)
    return (values[0] - 8.0 * values[1] + 8.0 * values[3] - values[4]) / 12.0

def second_diff(padded, dimension):
    values = stencil_values(padded, dimension)
    return (-values[0] + 16.0 * values[1] - 30.0 * values[2] + 16.0 * values[3] - values[4]) / 12.0

def laplacian(padded):
    return second_diff(padded, 1) + second_diff(padded, 2) + second_diff(padded, 3)

def evolution(padded, mix_matrix, laplace_matrix):
    centre = interior(padded, 0)
    laplace = laplacian(padded)
    result = jnp.einsum('fg,gzyx->fzyx', mix_matrix, centre, precision=lax.Precision.HIGHEST)
    result = result + jnp.einsum('fg,gzyx->fzyx', laplace_matrix, laplace, precision=lax.Precision.HIGHEST)
    for dimension in (1, 2, 3):
        result = result + centre[11 + dimension][None] * first_diff(padded, dimension)
    return result

def contract(tensor, left, right):
    total = 0.0
    for first in range(3):
        for second in range(3):
            total = total + tensor[first][second] * left[first] * right[second]
    return total

def weyl_scalar(padded, zpos, ypos, xpos):
    table = ((0, 1, 2), (1, 3, 4), (2, 4, 5))
    metric = padded[0:6]
    curv_padded = padded[6:12]
    lap_metric = laplacian(metric)
    curvature = interior(curv_padded, 0)
    gradient = [first_diff(curv_padded, 3 - index) for index in range(3)]
    trace = curvature[0] + curvature[3] + curvature[5]
    electric = []
    curl = []
    for first in range(3):
        erow = []
        crow = []
        for second in range(3):
            value = -0.5 * lap_metric[table[first][second]] - trace * curvature[table[first][second]]
            for middle in range(3):
                value = value + curvature[table[first][middle]] * curvature[table[middle][second]]
            erow.append(value)
            next_one = (first + 1) % 3
            next_two = (first + 2) % 3
            crow.append(gradient[next_one][table[next_two][second]] - gradient[next_two][table[next_one][second]])
        electric.append(erow)
        curl.append(crow)
    magnetic = [[0.5 * (curl[first][second] + curl[second][first]) for second in range(3)] for first in range(3)]
    along_x = xpos[None, None, :]
    along_y = ypos[None, :, None]
    along_z = zpos[:, None, None]
    cylinder = jnp.sqrt(along_x * along_x + along_y * along_y)
    radius = jnp.sqrt(cylinder * cylinder + along_z * along_z)
    theta_vec = (along_z * along_x / (radius * cylinder), along_z * along_y / (radius * cylinder), -cylinder / radius)
    phi_vec = (-along_y / cylinder, along_x / cylinder, 0.0)
    real_part = 0.5 * (contract(electric, theta_vec, theta_vec) - contract(electric, phi_vec, phi_vec)) - contract(magnetic, theta_vec, phi_vec)
    imag_part = -contract(electric, theta_vec, phi_vec) - 0.5 * (contract(magnetic, theta_vec, theta_vec) - contract(magnetic, phi_vec, phi_vec))
    shape = curvature.shape[1:]
    return jnp.stack([jnp.broadcast_to(real_part, shape), jnp.broadcast_to(imag_part, shape)])

def centred(index, count):
    return index.astype(jnp.float32) + 0.5 - 0.5 * count

def reference(fields, mix_matrix, laplace_matrix):
    rows = fields.shape[2]
    width = fields.shape[3]
    padded = pad_periodic(pad_periodic(pad_periodic(fields, 1), 2), 3)
    ypos = centred(jnp.arange(rows, dtype=jnp.int32), rows)
    xpos = centred(jnp.arange(width, dtype=jnp.int32), width)

    def block(index):
        start = (index * CZ).astype(jnp.int32)
        window = lax.dynamic_slice_in_dim(padded, start, CZ + 4, axis=1)
        zpos = centred(start + jnp.arange(CZ, dtype=jnp.int32), NZ)
        return (evolution(window, mix_matrix, laplace_matrix), weyl_scalar(window[0:12], zpos, ypos, xpos))
    rhs_blocks, weyl_blocks = lax.map(block, jnp.arange(NZ // CZ, dtype=jnp.int32))
    rhs = jnp.transpose(rhs_blocks, (1, 0, 2, 3, 4)).reshape(FIELDS, NZ, rows, width)
    weyl = jnp.transpose(weyl_blocks, (1, 0, 2, 3, 4)).reshape(2, NZ, rows, width)
    return (rhs, weyl)
```

```python
import functools

import jax
import jax.numpy as jnp
from jax import lax
from jax.experimental import pallas as pl
from jax.experimental.pallas import tpu as pltpu
from jax.sharding import PartitionSpec as P


CHUNKS = 4
WEYL_FIELDS = 12
FIRST = {-2: 1.0 / 12.0, -1: -8.0 / 12.0, 1: 8.0 / 12.0, 2: -1.0 / 12.0}
SECOND = {-2: -1.0 / 12.0, -1: 16.0 / 12.0, 0: -30.0 / 12.0, 1: 16.0 / 12.0, 2: -1.0 / 12.0}
TABLE = ((0, 1, 2), (1, 3, 4), (2, 4, 5))
SMEM = functools.partial(pl.BlockSpec, memory_space=pltpu.SMEM)


def plus(left, right):
    if left is None:
        return right
    if right is None:
        return left
    return left + right


def minus(left, right):
    if right is None:
        return left
    if left is None:
        return -right
    return left - right


def weights(zpos, row, shape, ny, nx):
    along_x = lax.broadcasted_iota(jnp.int32, shape, 1).astype(jnp.float32) + (0.5 - 0.5 * nx)
    along_y = (lax.broadcasted_iota(jnp.int32, shape, 0) + row).astype(jnp.float32)
    along_y = along_y + (0.5 - 0.5 * ny)
    square = along_x * along_x + along_y * along_y
    cylinder = jnp.sqrt(square)
    radius = jnp.sqrt(square + zpos * zpos)
    over_s = 1.0 / cylinder
    over_r = 1.0 / radius
    cos = along_x * over_s
    sin = along_y * over_s
    zed = zpos * over_r
    theta = (zed * cos, zed * sin, -cylinder * over_r)
    phi = (-sin, cos, None)
    even = {}
    odd = {}
    for i in range(3):
        for j in range(i, 3):
            scale = 0.5 if i == j else 1.0
            value = theta[i] * theta[j]
            if phi[i] is not None and phi[j] is not None:
                value = value - phi[i] * phi[j]
            even[TABLE[i][j]] = scale * value
            value = None
            if phi[j] is not None:
                value = plus(value, theta[i] * phi[j])
            if phi[i] is not None:
                value = plus(value, theta[j] * phi[i])
            odd[TABLE[i][j]] = None if value is None else scale * value
    return even, odd


def project(tensor, weight):
    total = None
    for index in range(6):
        if tensor[index] is not None and weight[index] is not None:
            total = plus(total, tensor[index] * weight[index])
    return total


def scalar_pair(electric, grad, even, odd):
    curl = []
    for first in range(3):
        row = []
        up = (first + 1) % 3
        down = (first + 2) % 3
        for second in range(3):
            left = None if grad[up] is None else grad[up][TABLE[down][second]]
            right = None if grad[down] is None else grad[down][TABLE[up][second]]
            row.append(minus(left, right))
        curl.append(row)
    magnetic = {}
    for i in range(3):
        for j in range(i, 3):
            if i == j:
                magnetic[TABLE[i][j]] = curl[i][i]
            else:
                value = plus(curl[i][j], curl[j][i])
                magnetic[TABLE[i][j]] = None if value is None else 0.5 * value
    real = project(electric, even) - project(magnetic, odd)
    imag = -project(electric, odd) - project(magnetic, even)
    return real, imag


def local_kernel(fields_ref, zbase_ref, lap_ref, acc_ref, weyl_ref, gx_ref, gy_ref):
    count, depth, ny, nx = fields_ref.shape

    def derive(keep, g, carry):
        for z in range(depth):
            f = fields_ref[g, z]
            parts = []
            for axis, size in ((1, nx), (0, ny)):
                a1 = pltpu.roll(f, 1, axis)
                b1 = pltpu.roll(f, size - 1, axis)
                a2 = pltpu.roll(f, 2, axis)
                b2 = pltpu.roll(f, size - 2, axis)
                d1 = (8.0 / 12.0) * (b1 - a1) + (1.0 / 12.0) * (a2 - b2)
                d2 = (16.0 / 12.0) * (b1 + a1) - (1.0 / 12.0) * (a2 + b2)
                parts.append((d1, d2))
            lap = parts[0][1] + parts[1][1] - 7.5 * f
            adv = fields_ref[14, z] * parts[0][0] + fields_ref[13, z] * parts[1][0]
            dz = None
            for offset in (-2, -1, 1, 2):
                if 0 <= z + offset < depth:
                    other = fields_ref[g, z + offset]
                    lap = lap + SECOND[offset] * other
                    dz = plus(dz, FIRST[offset] * other)
            if dz is not None:
                adv = adv + fields_ref[12, z] * dz
            lap_ref[g, z] = lap
            acc_ref[g, z] = adv
            if keep:
                gx_ref[g - 6, z] = parts[0][0]
                gy_ref[g - 6, z] = parts[1][0]
        return carry

    lax.fori_loop(0, 6, functools.partial(derive, False), 0)
    lax.fori_loop(6, 12, functools.partial(derive, True), 0)
    lax.fori_loop(12, count, functools.partial(derive, False), 0)

    tile = 16
    for z in range(depth):
        def weyl_tile(t, carry, z=z):
            row = pl.multiple_of(t * tile, tile)
            rows = pl.ds(row, tile)
            even, odd = weights(zbase_ref[0] + float(z), row, (tile, nx), ny, nx)
            curv = [fields_ref[6 + i, z, rows, :] for i in range(6)]
            trace = curv[0] + curv[3] + curv[5]
            electric = {}
            for i in range(3):
                for j in range(i, 3):
                    index = TABLE[i][j]
                    value = -0.5 * lap_ref[index, z, rows, :] - trace * curv[index]
                    for m in range(3):
                        value = value + curv[TABLE[i][m]] * curv[TABLE[m][j]]
                    electric[index] = value
            along_z = None
            for offset in (-2, -1, 1, 2):
                if 0 <= z + offset < depth:
                    term = [FIRST[offset] * fields_ref[6 + i, z + offset, rows, :] for i in range(6)]
                    along_z = term if along_z is None else [a + b for a, b in zip(along_z, term)]
            grad = [
                [gx_ref[i, z, rows, :] for i in range(6)],
                [gy_ref[i, z, rows, :] for i in range(6)],
                along_z,
            ]
            real, imag = scalar_pair(electric, grad, even, odd)
            weyl_ref[0, z, rows, :] = real
            weyl_ref[1, z, rows, :] = imag
            return carry

        lax.fori_loop(0, ny // tile, weyl_tile, 0)


def mix_kernel(mix_ref, lapm_ref, fields_ref, lap_ref, acc_ref, out_ref):
    count = fields_ref.shape[0]
    block = 6
    for base in range(0, count, block):
        totals = [acc_ref[base + c, 0] for c in range(block)]
        for g in range(count):
            f = fields_ref[g, 0]
            lap = lap_ref[g, 0]
            for c in range(block):
                at = (base + c) * count + g
                totals[c] = totals[c] + (mix_ref[at] * f + lapm_ref[at] * lap)
        for c in range(block):
            out_ref[base + c, 0] = totals[c]


def sides(first_ref, second_ref, parity, g, z, depth):
    found = []
    for offset in (-2, -1, 1, 2):
        at = z + offset
        if 0 <= at < depth:
            continue
        if at < 0:
            value = jnp.where(parity, first_ref[g, depth + at], second_ref[g, depth + at])
        else:
            value = jnp.where(parity, second_ref[g, at - depth], first_ref[g, at - depth])
        found.append((offset, value))
    return found


def weighted(found, coefficients):
    total = None
    for offset, value in found:
        total = plus(total, coefficients[offset] * value)
    return total


def halo_kernel(starts, parity_ref, lapm_ref, beta_ref, acc_ref, *refs):
    out_ref = refs[-1]
    count, depth = acc_ref.shape[:2]
    parity = parity_ref[0] == 1
    for z in range(depth):
        second = []
        first = {}
        for k, start in enumerate(starts):
            r1, r2 = refs[2 * k], refs[2 * k + 1]
            for g in range(r1.shape[0]):
                found = sides(r1, r2, parity, g, z, depth)
                if found:
                    second.append((start + g, weighted(found, SECOND)))
                    first[start + g] = beta_ref[0, z] * weighted(found, FIRST)
        for c in range(count):
            total = acc_ref[c, z]
            if c in first:
                total = total + first[c]
            for g, value in second:
                total = total + lapm_ref[c * count + g] * value
            out_ref[c, z] = total


def weyl_kernel(starts, ny, parity_ref, zbase_ref, local_ref, *refs):
    out_ref = refs[-1]
    depth, tile, nx = local_ref.shape[1:]
    parity = parity_ref[0] == 1
    row = pl.program_id(0) * tile
    where = {}
    for k, start in enumerate(starts):
        for g in range(refs[2 * k].shape[0]):
            where[start + g] = (refs[2 * k], refs[2 * k + 1], g)
    for z in range(depth):
        even, odd = weights(zbase_ref[0] + float(z), row, (tile, nx), ny, nx)
        electric = {}
        along_z = []
        for i in range(6):
            r1, r2, g = where[i]
            electric[i] = -0.5 * weighted(sides(r1, r2, parity, g, z, depth), SECOND)
            r1, r2, g = where[6 + i]
            along_z.append(weighted(sides(r1, r2, parity, g, z, depth), FIRST))
        real, imag = scalar_pair(electric, [None, None, along_z], even, odd)
        out_ref[0, z] = local_ref[0, z] + real
        out_ref[1, z] = local_ref[1, z] + imag


def local_part(fields, zbase):
    count, depth, ny, nx = fields.shape
    whole = jax.ShapeDtypeStruct(fields.shape, fields.dtype)
    return pl.pallas_call(
        local_kernel,
        out_shape=(whole, whole, jax.ShapeDtypeStruct((2, depth, ny, nx), fields.dtype)),
        in_specs=[pl.BlockSpec(memory_space=pltpu.VMEM), SMEM()],
        out_specs=[pl.BlockSpec(memory_space=pltpu.VMEM)] * 3,
        scratch_shapes=[pltpu.VMEM((6, depth, ny, nx), fields.dtype)] * 2,
        name="local_part",
    )(fields, zbase)


def mix_part(mix, lapm, fields, lap, acc):
    count, depth, ny, nx = fields.shape
    tile = 32 if ny % 32 == 0 else 8
    spec = pl.BlockSpec((count, 1, tile, nx), lambda z, t: (0, z, t, 0))
    return pl.pallas_call(
        mix_kernel,
        grid=(depth, ny // tile),
        out_shape=jax.ShapeDtypeStruct(fields.shape, fields.dtype),
        in_specs=[SMEM(), SMEM(), spec, spec, spec],
        out_specs=spec,
        name="mix_part",
    )(mix, lapm, fields, lap, acc)


def halo_part(starts, parity, lapm, fields, acc, pieces):
    count, depth, ny, nx = fields.shape
    tile = 16 if ny % 16 == 0 else 8
    spec = pl.BlockSpec((count, depth, tile, nx), lambda t: (0, 0, t, 0))
    in_specs = [SMEM(), SMEM(), pl.BlockSpec((1, depth, tile, nx), lambda t: (12, 0, t, 0)), spec]
    for piece in pieces:
        in_specs.append(pl.BlockSpec((piece.shape[0], depth, tile, nx), lambda t: (0, 0, t, 0)))
    return pl.pallas_call(
        functools.partial(halo_kernel, starts),
        grid=(ny // tile,),
        out_shape=jax.ShapeDtypeStruct(fields.shape, fields.dtype),
        in_specs=in_specs,
        out_specs=spec,
        name="halo_part",
    )(parity, lapm, fields, acc, *pieces)


def weyl_part(starts, parity, zbase, local, pieces):
    _, depth, ny, nx = local.shape
    tile = 16 if ny % 16 == 0 else 8
    spec = pl.BlockSpec((2, depth, tile, nx), lambda t: (0, 0, t, 0))
    in_specs = [SMEM(), SMEM(), spec]
    for piece in pieces:
        in_specs.append(pl.BlockSpec((piece.shape[0], depth, tile, nx), lambda t: (0, 0, t, 0)))
    return pl.pallas_call(
        functools.partial(weyl_kernel, starts, ny),
        grid=(ny // tile,),
        out_shape=jax.ShapeDtypeStruct(local.shape, local.dtype),
        in_specs=in_specs,
        out_specs=spec,
        name="weyl_part",
    )(parity, zbase, local, *pieces)


def per_device(fields, mix_matrix, laplace_matrix):
    count, depth, ny, nx = fields.shape
    groups = lax.axis_size("grp")
    members = lax.axis_size("dev")
    ring = groups * members
    axes = ("grp", "dev")
    slab = lax.axis_index("grp") * members + lax.axis_index("dev")
    swap = [(i, i + 1 - 2 * (i % 2)) for i in range(ring)]
    onward = [(i, (i + 2 - 4 * (i % 2)) % ring) for i in range(ring)]
    size = count // CHUNKS
    starts = list(range(0, count, size))
    pieces = []
    for start in starts:
        mine = lax.slice_in_dim(fields, start, start + size, axis=0)
        beside = lax.ppermute(mine, axes, swap)
        pieces.append((beside, lax.ppermute(beside, axes, onward)))
    parity = (slab % 2).astype(jnp.int32).reshape(1)
    zbase = ((slab * depth).astype(jnp.float32) + (0.5 - 0.5 * depth * ring)).reshape(1)
    mix = mix_matrix.reshape(-1)
    lapm = laplace_matrix.reshape(-1)
    lap, acc, local = local_part(fields, zbase)
    acc = mix_part(mix, lapm, fields, lap, acc)
    early = [k for k, start in enumerate(starts) if start < WEYL_FIELDS]
    flat = [piece for k in early for piece in pieces[k]]
    weyl = weyl_part([starts[k] for k in early], parity, zbase, local, flat)
    weyl = lax.all_to_all(weyl, "dev", split_axis=2, concat_axis=1, tiled=True)
    groups_of = [early] + [[k] for k in range(len(early), len(starts))]
    for group in groups_of:
        flat = [piece for k in group for piece in pieces[k]]
        acc = halo_part([starts[k] for k in group], parity, lapm, fields, acc, flat)
    return (acc, weyl)


def solution(mesh):
    return jax.shard_map(
        per_device,
        mesh=mesh,
        in_specs=(P(None, ("grp", "dev"), None, None), P(), P()),
        out_specs=(P(None, ("grp", "dev"), None, None), P(None, "grp", "dev", None)),
        check_vma=False,
    )
```

```python
import functools

import jax
import jax.numpy as jnp
from jax import lax
from jax.experimental import pallas as pl
from jax.experimental.pallas import tpu as pltpu
from jax.sharding import PartitionSpec as P


WEYL_FIELDS = 12
FIRST = {-2: 1.0 / 12.0, -1: -8.0 / 12.0, 1: 8.0 / 12.0, 2: -1.0 / 12.0}
SECOND = {-2: -1.0 / 12.0, -1: 16.0 / 12.0, 0: -30.0 / 12.0, 1: 16.0 / 12.0, 2: -1.0 / 12.0}
TABLE = ((0, 1, 2), (1, 3, 4), (2, 4, 5))
SMEM = functools.partial(pl.BlockSpec, memory_space=pltpu.SMEM)


def plus(left, right):
    if left is None:
        return right
    if right is None:
        return left
    return left + right


def minus(left, right):
    if right is None:
        return left
    if left is None:
        return -right
    return left - right


def weights(zpos, row, shape, ny, nx):
    along_x = lax.broadcasted_iota(jnp.int32, shape, 1).astype(jnp.float32) + (0.5 - 0.5 * nx)
    along_y = (lax.broadcasted_iota(jnp.int32, shape, 0) + row).astype(jnp.float32)
    along_y = along_y + (0.5 - 0.5 * ny)
    square = along_x * along_x + along_y * along_y
    cylinder = jnp.sqrt(square)
    radius = jnp.sqrt(square + zpos * zpos)
    over_s = 1.0 / cylinder
    over_r = 1.0 / radius
    cos = along_x * over_s
    sin = along_y * over_s
    zed = zpos * over_r
    theta = (zed * cos, zed * sin, -cylinder * over_r)
    phi = (-sin, cos, None)
    even = {}
    odd = {}
    for i in range(3):
        for j in range(i, 3):
            scale = 0.5 if i == j else 1.0
            value = theta[i] * theta[j]
            if phi[i] is not None and phi[j] is not None:
                value = value - phi[i] * phi[j]
            even[TABLE[i][j]] = scale * value
            value = None
            if phi[j] is not None:
                value = plus(value, theta[i] * phi[j])
            if phi[i] is not None:
                value = plus(value, theta[j] * phi[i])
            odd[TABLE[i][j]] = None if value is None else scale * value
    return even, odd


def project(tensor, weight):
    total = None
    for index in range(6):
        if tensor[index] is not None and weight[index] is not None:
            total = plus(total, tensor[index] * weight[index])
    return total


def scalar_pair(electric, grad, even, odd):
    curl = []
    for first in range(3):
        row = []
        up = (first + 1) % 3
        down = (first + 2) % 3
        for second in range(3):
            left = None if grad[up] is None else grad[up][TABLE[down][second]]
            right = None if grad[down] is None else grad[down][TABLE[up][second]]
            row.append(minus(left, right))
        curl.append(row)
    magnetic = {}
    for i in range(3):
        for j in range(i, 3):
            if i == j:
                magnetic[TABLE[i][j]] = curl[i][i]
            else:
                value = plus(curl[i][j], curl[j][i])
                magnetic[TABLE[i][j]] = None if value is None else 0.5 * value
    real = project(electric, even) - project(magnetic, odd)
    imag = -project(electric, odd) - project(magnetic, even)
    return real, imag


def local_kernel(fields_ref, beta_ref, zbase_ref, lap_ref, acc_ref, weyl_ref, hess_ref, gx_ref, gy_ref):
    count, depth, ny, nx = fields_ref.shape
    step = pl.program_id(0)

    def derive(g, carry):
        for z in range(depth):
            f = fields_ref[g, z]
            parts = []
            for axis, size in ((1, nx), (0, ny)):
                a1 = pltpu.roll(f, 1, axis)
                b1 = pltpu.roll(f, size - 1, axis)
                a2 = pltpu.roll(f, 2, axis)
                b2 = pltpu.roll(f, size - 2, axis)
                d1 = (8.0 / 12.0) * (b1 - a1) + (1.0 / 12.0) * (a2 - b2)
                d2 = (16.0 / 12.0) * (b1 + a1) - (1.0 / 12.0) * (a2 + b2)
                parts.append((d1, d2))
            lap = parts[0][1] + parts[1][1] - 7.5 * f
            adv = beta_ref[2, z] * parts[0][0] + beta_ref[1, z] * parts[1][0]
            dz = None
            for offset in (-2, -1, 1, 2):
                if 0 <= z + offset < depth:
                    other = fields_ref[g, z + offset]
                    lap = lap + SECOND[offset] * other
                    dz = plus(dz, FIRST[offset] * other)
            if dz is not None:
                adv = adv + beta_ref[0, z] * dz
            lap_ref[g, z] = lap
            acc_ref[g, z] = adv

            @pl.when(step == 0)
            def _():
                hess_ref[g, z] = lap

            @pl.when(step == 1)
            def _():
                gx_ref[g, z] = parts[0][0]
                gy_ref[g, z] = parts[1][0]
        return carry

    lax.fori_loop(0, count, derive, 0)

    tile = 16 if ny % 16 == 0 else 8

    @pl.when(step == 1)
    def _():
        for z in range(depth):
            def weyl_tile(t, carry, z=z):
                row = pl.multiple_of(t * tile, tile)
                rows = pl.ds(row, tile)
                even, odd = weights(zbase_ref[0] + float(z), row, (tile, nx), ny, nx)
                curv = [fields_ref[i, z, rows, :] for i in range(6)]
                trace = curv[0] + curv[3] + curv[5]
                electric = {}
                for i in range(3):
                    for j in range(i, 3):
                        index = TABLE[i][j]
                        value = -0.5 * hess_ref[index, z, rows, :] - trace * curv[index]
                        for m in range(3):
                            value = value + curv[TABLE[i][m]] * curv[TABLE[m][j]]
                        electric[index] = value
                along_z = None
                for offset in (-2, -1, 1, 2):
                    if 0 <= z + offset < depth:
                        term = [FIRST[offset] * fields_ref[i, z + offset, rows, :] for i in range(6)]
                        along_z = term if along_z is None else [p + q for p, q in zip(along_z, term)]
                grad = [
                    [gx_ref[i, z, rows, :] for i in range(6)],
                    [gy_ref[i, z, rows, :] for i in range(6)],
                    along_z,
                ]
                real, imag = scalar_pair(electric, grad, even, odd)
                weyl_ref[0, z, rows, :] = real
                weyl_ref[1, z, rows, :] = imag
                return carry

            lax.fori_loop(0, ny // tile, weyl_tile, 0)


def sides(first_ref, second_ref, parity, g, z, depth):
    found = []
    for offset in (-2, -1, 1, 2):
        at = z + offset
        if 0 <= at < depth:
            continue
        if at < 0:
            value = jnp.where(parity, first_ref[g, depth + at], second_ref[g, depth + at])
        else:
            value = jnp.where(parity, second_ref[g, at - depth], first_ref[g, at - depth])
        found.append((offset, value))
    return found


def weighted(found, coefficients):
    total = None
    for offset, value in found:
        total = plus(total, coefficients[offset] * value)
    return total


def halo_kernel(starts, parity_ref, lapm_ref, beta_ref, acc_ref, *refs):
    out_ref = refs[-1]
    count, depth = acc_ref.shape[:2]
    parity = parity_ref[0] == 1
    for z in range(depth):
        second = []
        first = {}
        for k, start in enumerate(starts):
            r1, r2 = refs[2 * k], refs[2 * k + 1]
            for g in range(r1.shape[0]):
                found = sides(r1, r2, parity, g, z, depth)
                if found:
                    second.append((start + g, weighted(found, SECOND)))
                    first[start + g] = beta_ref[0, z] * weighted(found, FIRST)
        for c in range(count):
            total = acc_ref[c, z]
            if c in first:
                total = total + first[c]
            for g, value in second:
                total = total + lapm_ref[c * count + g] * value
            out_ref[c, z] = total


def weyl_kernel(ny, row0, parity_ref, zbase_ref, local_ref, r1, r2, out_ref):
    depth, tile, nx = local_ref.shape[1:]
    parity = parity_ref[0] == 1
    row = row0 + pl.program_id(0) * tile
    for z in range(depth):
        even, odd = weights(zbase_ref[0] + float(z), row, (tile, nx), ny, nx)
        electric = {}
        along_z = []
        for i in range(6):
            electric[i] = -0.5 * weighted(sides(r1, r2, parity, i, z, depth), SECOND)
            along_z.append(weighted(sides(r1, r2, parity, 6 + i, z, depth), FIRST))
        real, imag = scalar_pair(electric, [None, None, along_z], even, odd)
        out_ref[0, z] = local_ref[0, z] + real
        out_ref[1, z] = local_ref[1, z] + imag


def local_part(fields, zbase):
    count, depth, ny, nx = fields.shape
    whole = jax.ShapeDtypeStruct(fields.shape, fields.dtype)
    spec = pl.BlockSpec((6, depth, ny, nx), lambda g: (g, 0, 0, 0))
    return pl.pallas_call(
        local_kernel,
        grid=(count // 6,),
        out_shape=(whole, whole, jax.ShapeDtypeStruct((2, depth, ny, nx), fields.dtype)),
        in_specs=[spec, pl.BlockSpec((3, depth, ny, nx), lambda g: (4, 0, 0, 0)), SMEM()],
        out_specs=[spec, spec, pl.BlockSpec((2, depth, ny, nx), lambda g: (0, 0, 0, 0))],
        scratch_shapes=[pltpu.VMEM((6, depth, ny, nx), fields.dtype)] * 3,
        name="local_part",
    )(fields, fields, zbase)


def halo_part(starts, row0, rows, parity, lapm, fields, acc, pieces):
    count, depth, _, nx = fields.shape
    tile = 16 if row0 % 16 == 0 and rows % 16 == 0 else 8
    at = row0 // tile
    spec = pl.BlockSpec((count, depth, tile, nx), lambda t: (0, 0, at + t, 0))
    in_specs = [SMEM(), SMEM(), pl.BlockSpec((1, depth, tile, nx), lambda t: (12, 0, at + t, 0)), spec]
    for piece in pieces:
        in_specs.append(pl.BlockSpec((piece.shape[0], depth, tile, nx), lambda t: (0, 0, t, 0)))
    return pl.pallas_call(
        functools.partial(halo_kernel, starts),
        grid=(rows // tile,),
        out_shape=jax.ShapeDtypeStruct(fields.shape, fields.dtype),
        in_specs=in_specs,
        out_specs=spec,
        input_output_aliases={3: 0},
        name="halo_part",
    )(parity, lapm, fields, acc, *pieces)


def weyl_part(row0, rows, parity, zbase, local, pieces):
    _, depth, ny, nx = local.shape
    tile = 16 if row0 % 16 == 0 and rows % 16 == 0 else 8
    at = row0 // tile
    spec = pl.BlockSpec((2, depth, tile, nx), lambda t: (0, 0, at + t, 0))
    in_specs = [SMEM(), SMEM(), spec]
    for piece in pieces:
        in_specs.append(pl.BlockSpec((piece.shape[0], depth, tile, nx), lambda t: (0, 0, t, 0)))
    return pl.pallas_call(
        functools.partial(weyl_kernel, ny, row0),
        grid=(rows // tile,),
        out_shape=jax.ShapeDtypeStruct(local.shape, local.dtype),
        in_specs=in_specs,
        out_specs=spec,
        input_output_aliases={2: 0},
        name="weyl_part",
    )(parity, zbase, local, *pieces)


def row_ranges(ny):
    unit = ny // 8
    return [(0, 2 * unit), (2 * unit, 3 * unit), (5 * unit, 3 * unit)]


def per_device(fields, mix_matrix, laplace_matrix):
    count, depth, ny, nx = fields.shape
    groups = lax.axis_size("grp")
    members = lax.axis_size("dev")
    ring = groups * members
    axes = ("grp", "dev")
    slab = lax.axis_index("grp") * members + lax.axis_index("dev")
    swap = [(i, i + 1 - 2 * (i % 2)) for i in range(ring)]
    onward = [(i, (i + 2 - 4 * (i % 2)) % ring) for i in range(ring)]
    ranges = row_ranges(ny)
    order = [(0, WEYL_FIELDS, j) for j in range(len(ranges))]
    order += [(WEYL_FIELDS, count, j) for j in reversed(range(len(ranges)))]
    pieces = {}
    for begin, end, j in order:
        row0, rows = ranges[j]
        mine = lax.slice(fields, (begin, 0, row0, 0), (end, depth, row0 + rows, nx))
        beside = lax.ppermute(mine, axes, swap)
        pieces[begin, j] = [beside, lax.ppermute(beside, axes, onward)]
    parity = (slab % 2).astype(jnp.int32).reshape(1)
    zbase = ((slab * depth).astype(jnp.float32) + (0.5 - 0.5 * depth * ring)).reshape(1)
    lapm = laplace_matrix.reshape(-1)
    lap, acc, weyl = local_part(fields, zbase)
    acc = acc + (
        jnp.einsum("fg,gzyx->fzyx", mix_matrix, fields, precision=lax.Precision.HIGH)
        + jnp.einsum("fg,gzyx->fzyx", laplace_matrix, lap, precision=lax.Precision.HIGH)
    )
    for j, (row0, rows) in enumerate(ranges):
        weyl = weyl_part(row0, rows, parity, zbase, weyl, pieces[0, j])
    weyl = lax.all_to_all(weyl, "dev", split_axis=2, concat_axis=1, tiled=True)
    for j in reversed(range(len(ranges))):
        row0, rows = ranges[j]
        flat = pieces[0, j] + pieces[WEYL_FIELDS, j]
        acc = halo_part([0, WEYL_FIELDS], row0, rows, parity, lapm, fields, acc, flat)
    return (acc, weyl)


def solution(mesh):
    return jax.shard_map(
        per_device,
        mesh=mesh,
        in_specs=(P(None, ("grp", "dev"), None, None), P(), P()),
        out_specs=(P(None, ("grp", "dev"), None, None), P(None, "grp", "dev", None)),
        check_vma=False,
    )
```

```python
import functools

import jax
import jax.numpy as jnp
from jax import lax
from jax.experimental import pallas as pl
from jax.experimental.pallas import tpu as pltpu
from jax.sharding import PartitionSpec as P


WEYL_FIELDS = 12
FIRST = {-2: 1.0 / 12.0, -1: -8.0 / 12.0, 1: 8.0 / 12.0, 2: -1.0 / 12.0}
SECOND = {-2: -1.0 / 12.0, -1: 16.0 / 12.0, 0: -30.0 / 12.0, 1: 16.0 / 12.0, 2: -1.0 / 12.0}
TABLE = ((0, 1, 2), (1, 3, 4), (2, 4, 5))
SMEM = functools.partial(pl.BlockSpec, memory_space=pltpu.SMEM)


def plus(left, right):
    if left is None:
        return right
    if right is None:
        return left
    return left + right


def minus(left, right):
    if right is None:
        return left
    if left is None:
        return -right
    return left - right


def weights(zpos, row, shape, ny, nx):
    along_x = lax.broadcasted_iota(jnp.int32, shape, 1).astype(jnp.float32) + (0.5 - 0.5 * nx)
    along_y = (lax.broadcasted_iota(jnp.int32, shape, 0) + row).astype(jnp.float32)
    along_y = along_y + (0.5 - 0.5 * ny)
    square = along_x * along_x + along_y * along_y
    cylinder = jnp.sqrt(square)
    radius = jnp.sqrt(square + zpos * zpos)
    over_s = 1.0 / cylinder
    over_r = 1.0 / radius
    cos = along_x * over_s
    sin = along_y * over_s
    zed = zpos * over_r
    theta = (zed * cos, zed * sin, -cylinder * over_r)
    phi = (-sin, cos, None)
    even = {}
    odd = {}
    for i in range(3):
        for j in range(i, 3):
            scale = 0.5 if i == j else 1.0
            value = theta[i] * theta[j]
            if phi[i] is not None and phi[j] is not None:
                value = value - phi[i] * phi[j]
            even[TABLE[i][j]] = scale * value
            value = None
            if phi[j] is not None:
                value = plus(value, theta[i] * phi[j])
            if phi[i] is not None:
                value = plus(value, theta[j] * phi[i])
            odd[TABLE[i][j]] = None if value is None else scale * value
    return even, odd


def project(tensor, weight):
    total = None
    for index in range(6):
        if tensor[index] is not None and weight[index] is not None:
            total = plus(total, tensor[index] * weight[index])
    return total


def scalar_pair(electric, grad, even, odd):
    curl = []
    for first in range(3):
        row = []
        up = (first + 1) % 3
        down = (first + 2) % 3
        for second in range(3):
            left = None if grad[up] is None else grad[up][TABLE[down][second]]
            right = None if grad[down] is None else grad[down][TABLE[up][second]]
            row.append(minus(left, right))
        curl.append(row)
    magnetic = {}
    for i in range(3):
        for j in range(i, 3):
            if i == j:
                magnetic[TABLE[i][j]] = curl[i][i]
            else:
                value = plus(curl[i][j], curl[j][i])
                magnetic[TABLE[i][j]] = None if value is None else 0.5 * value
    real = project(electric, even) - project(magnetic, odd)
    imag = -project(electric, odd) - project(magnetic, even)
    return real, imag


def local_kernel(fields_ref, beta_ref, zbase_ref, lap_ref, acc_ref, weyl_ref, hess_ref, gx_ref, gy_ref):
    count, depth, ny, nx = fields_ref.shape
    step = pl.program_id(0)

    def derive(g, carry):
        for z in range(depth):
            f = fields_ref[g, z]
            parts = []
            for axis, size in ((1, nx), (0, ny)):
                a1 = pltpu.roll(f, 1, axis)
                b1 = pltpu.roll(f, size - 1, axis)
                a2 = pltpu.roll(f, 2, axis)
                b2 = pltpu.roll(f, size - 2, axis)
                d1 = (8.0 / 12.0) * (b1 - a1) + (1.0 / 12.0) * (a2 - b2)
                d2 = (16.0 / 12.0) * (b1 + a1) - (1.0 / 12.0) * (a2 + b2)
                parts.append((d1, d2))
            lap = parts[0][1] + parts[1][1] - 7.5 * f
            adv = beta_ref[2, z] * parts[0][0] + beta_ref[1, z] * parts[1][0]
            dz = None
            for offset in (-2, -1, 1, 2):
                if 0 <= z + offset < depth:
                    other = fields_ref[g, z + offset]
                    lap = lap + SECOND[offset] * other
                    dz = plus(dz, FIRST[offset] * other)
            if dz is not None:
                adv = adv + beta_ref[0, z] * dz
            lap_ref[g, z] = lap
            acc_ref[g, z] = adv

            @pl.when(step == 0)
            def _():
                hess_ref[g, z] = lap

            @pl.when(step == 1)
            def _():
                gx_ref[g, z] = parts[0][0]
                gy_ref[g, z] = parts[1][0]
        return carry

    lax.fori_loop(0, count, derive, 0)

    tile = 16 if ny % 16 == 0 else 8

    @pl.when(step == 1)
    def _():
        for z in range(depth):
            def weyl_tile(t, carry, z=z):
                row = pl.multiple_of(t * tile, tile)
                rows = pl.ds(row, tile)
                even, odd = weights(zbase_ref[0] + float(z), row, (tile, nx), ny, nx)
                curv = [fields_ref[i, z, rows, :] for i in range(6)]
                trace = curv[0] + curv[3] + curv[5]
                electric = {}
                for i in range(3):
                    for j in range(i, 3):
                        index = TABLE[i][j]
                        value = -0.5 * hess_ref[index, z, rows, :] - trace * curv[index]
                        for m in range(3):
                            value = value + curv[TABLE[i][m]] * curv[TABLE[m][j]]
                        electric[index] = value
                along_z = None
                for offset in (-2, -1, 1, 2):
                    if 0 <= z + offset < depth:
                        term = [FIRST[offset] * fields_ref[i, z + offset, rows, :] for i in range(6)]
                        along_z = term if along_z is None else [p + q for p, q in zip(along_z, term)]
                grad = [
                    [gx_ref[i, z, rows, :] for i in range(6)],
                    [gy_ref[i, z, rows, :] for i in range(6)],
                    along_z,
                ]
                real, imag = scalar_pair(electric, grad, even, odd)
                weyl_ref[0, z, rows, :] = real
                weyl_ref[1, z, rows, :] = imag
                return carry

            lax.fori_loop(0, ny // tile, weyl_tile, 0)


def sides(first_ref, second_ref, parity, g, z, depth):
    found = []
    for offset in (-2, -1, 1, 2):
        at = z + offset
        if 0 <= at < depth:
            continue
        if at < 0:
            value = jnp.where(parity, first_ref[g, depth + at], second_ref[g, depth + at])
        else:
            value = jnp.where(parity, second_ref[g, at - depth], first_ref[g, at - depth])
        found.append((offset, value))
    return found


def weighted(found, coefficients):
    total = None
    for offset, value in found:
        total = plus(total, coefficients[offset] * value)
    return total


def halo_kernel(starts, parity_ref, lapm_ref, beta_ref, acc_ref, *refs):
    out_ref = refs[-1]
    count, depth = acc_ref.shape[:2]
    parity = parity_ref[0] == 1
    for z in range(depth):
        second = []
        first = {}
        for k, start in enumerate(starts):
            r1, r2 = refs[2 * k], refs[2 * k + 1]
            for g in range(r1.shape[0]):
                found = sides(r1, r2, parity, g, z, depth)
                if found:
                    second.append((start + g, weighted(found, SECOND)))
                    first[start + g] = beta_ref[0, z] * weighted(found, FIRST)
        for c in range(count):
            total = acc_ref[c, z]
            if c in first:
                total = total + first[c]
            for g, value in second:
                total = total + lapm_ref[c * count + g] * value
            out_ref[c, z] = total


def weyl_kernel(ny, row0, parity_ref, zbase_ref, local_ref, r1, r2, out_ref):
    depth, tile, nx = local_ref.shape[1:]
    parity = parity_ref[0] == 1
    row = row0 + pl.program_id(0) * tile
    for z in range(depth):
        even, odd = weights(zbase_ref[0] + float(z), row, (tile, nx), ny, nx)
        electric = {}
        along_z = []
        for i in range(6):
            electric[i] = -0.5 * weighted(sides(r1, r2, parity, i, z, depth), SECOND)
            along_z.append(weighted(sides(r1, r2, parity, 6 + i, z, depth), FIRST))
        real, imag = scalar_pair(electric, [None, None, along_z], even, odd)
        out_ref[0, z] = local_ref[0, z] + real
        out_ref[1, z] = local_ref[1, z] + imag


def local_part(fields, zbase):
    count, depth, ny, nx = fields.shape
    whole = jax.ShapeDtypeStruct(fields.shape, fields.dtype)
    spec = pl.BlockSpec((6, depth, ny, nx), lambda g: (g, 0, 0, 0))
    return pl.pallas_call(
        local_kernel,
        grid=(count // 6,),
        out_shape=(whole, whole, jax.ShapeDtypeStruct((2, depth, ny, nx), fields.dtype)),
        in_specs=[spec, pl.BlockSpec((3, depth, ny, nx), lambda g: (4, 0, 0, 0)), SMEM()],
        out_specs=[spec, spec, pl.BlockSpec((2, depth, ny, nx), lambda g: (0, 0, 0, 0))],
        scratch_shapes=[pltpu.VMEM((6, depth, ny, nx), fields.dtype)] * 3,
        name="local_part",
    )(fields, fields, zbase)


def halo_part(starts, row0, rows, parity, lapm, fields, acc, pieces):
    count, depth, _, nx = fields.shape
    tile = 16 if row0 % 16 == 0 and rows % 16 == 0 else 8
    at = row0 // tile
    spec = pl.BlockSpec((count, depth, tile, nx), lambda t: (0, 0, at + t, 0))
    in_specs = [SMEM(), SMEM(), pl.BlockSpec((1, depth, tile, nx), lambda t: (12, 0, at + t, 0)), spec]
    for piece in pieces:
        in_specs.append(pl.BlockSpec((piece.shape[0], depth, tile, nx), lambda t: (0, 0, t, 0)))
    return pl.pallas_call(
        functools.partial(halo_kernel, starts),
        grid=(rows // tile,),
        out_shape=jax.ShapeDtypeStruct(fields.shape, fields.dtype),
        in_specs=in_specs,
        out_specs=spec,
        input_output_aliases={3: 0},
        name="halo_part",
    )(parity, lapm, fields, acc, *pieces)


def weyl_part(row0, rows, parity, zbase, local, pieces):
    _, depth, ny, nx = local.shape
    tile = 16 if row0 % 16 == 0 and rows % 16 == 0 else 8
    at = row0 // tile
    spec = pl.BlockSpec((2, depth, tile, nx), lambda t: (0, 0, at + t, 0))
    in_specs = [SMEM(), SMEM(), spec]
    for piece in pieces:
        in_specs.append(pl.BlockSpec((piece.shape[0], depth, tile, nx), lambda t: (0, 0, t, 0)))
    return pl.pallas_call(
        functools.partial(weyl_kernel, ny, row0),
        grid=(rows // tile,),
        out_shape=jax.ShapeDtypeStruct(local.shape, local.dtype),
        in_specs=in_specs,
        out_specs=spec,
        input_output_aliases={2: 0},
        name="weyl_part",
    )(parity, zbase, local, *pieces)


def row_ranges(ny):
    unit = ny // 8
    return [(0, 2 * unit), (2 * unit, 3 * unit), (5 * unit, 3 * unit)]


def per_device(fields, mix_matrix, laplace_matrix):
    count, depth, ny, nx = fields.shape
    groups = lax.axis_size("grp")
    members = lax.axis_size("dev")
    ring = groups * members
    axes = ("grp", "dev")
    slab = lax.axis_index("grp") * members + lax.axis_index("dev")
    swap = [(i, i + 1 - 2 * (i % 2)) for i in range(ring)]
    onward = [(i, (i + 2 - 4 * (i % 2)) % ring) for i in range(ring)]
    ranges = row_ranges(ny)
    order = [(0, WEYL_FIELDS, j) for j in range(len(ranges))]
    order += [(WEYL_FIELDS, count, j) for j in reversed(range(len(ranges)))]
    pieces = {}
    for begin, end, j in order:
        row0, rows = ranges[j]
        mine = lax.slice(fields, (begin, 0, row0, 0), (end, depth, row0 + rows, nx))
        beside = lax.ppermute(mine, axes, swap)
        pieces[begin, j] = [beside, lax.ppermute(beside, axes, onward)]
    parity = (slab % 2).astype(jnp.int32).reshape(1)
    zbase = ((slab * depth).astype(jnp.float32) + (0.5 - 0.5 * depth * ring)).reshape(1)
    lapm = laplace_matrix.reshape(-1)
    lap, acc, weyl = local_part(fields, zbase)
    mixed = jnp.einsum("fg,gzyx->fzyx", mix_matrix, fields, precision=lax.Precision.HIGH)
    acc = (acc + mixed) + jnp.einsum(
        "fg,gzyx->fzyx", laplace_matrix, lap, precision=lax.Precision.HIGH
    )
    for j, (row0, rows) in enumerate(ranges):
        weyl = weyl_part(row0, rows, parity, zbase, weyl, pieces[0, j])
    weyl = lax.all_to_all(weyl, "dev", split_axis=2, concat_axis=1, tiled=True)
    for j in reversed(range(len(ranges))):
        row0, rows = ranges[j]
        flat = pieces[0, j] + pieces[WEYL_FIELDS, j]
        acc = halo_part([0, WEYL_FIELDS], row0, rows, parity, lapm, fields, acc, flat)
    return (acc, weyl)


def solution(mesh):
    return jax.shard_map(
        per_device,
        mesh=mesh,
        in_specs=(P(None, ("grp", "dev"), None, None), P(), P()),
        out_specs=(P(None, ("grp", "dev"), None, None), P(None, "grp", "dev", None)),
        check_vma=False,
    )
```
